32 devices in a mesh: dp: 2 (over y), expert: 4 (over z), tensor: 4 (over x, core).
Axes of the slice: x: 2, y: 2, z: 4, core: 2. Of those that a mesh axis runs over, the one named last changes fastest.
Arguments:
- grad_out: bfloat16 [1024, 6144], P(('dp', 'expert'), 'tensor'), may hold values from -0.1875 to 0.1875
- expert_ids: int32 [1024, 2], P(('dp', 'expert')), may hold values from 0 to 3, all different within a row; in each aligned block of 128 rows (0 to 127, 128 to 255, ...) at most 64 rows name the same one
- route_gates: float32 [1024, 2], P(('dp', 'expert')), may hold values from 0.1 to 1
- saved_hidden: bfloat16 [4, 256, 16384], P('expert', 'dp', 'tensor'), may hold values from -6 to 6
Outputs:
- weight_grad: bfloat16 [4, 16384, 6144], P('expert', 'tensor', 'dp')
The draws below stay inside these ranges and needn't reach their ends.
Inputs may be any that keep to these rules, and one draw needn't show every extreme that they name: `expert_ids`: each row names 2 different experts. Among the rows of one device no expert is named by more than 64 rows, and every expert is named somewhere.
All inputs are finite; a program needn't handle non-finite values.
Results may differ from the reference program's by a relative error of at most 0.0049.
Values may be sent and summed in bfloat16 or wider, within the bound.
A program may use at most 128 MiB of HBM per device.

```python
import math
import jax
import jax.numpy as jnp
import numpy as np
from jax import lax

D = 6144
FF = 16384
TOP = 2
TOK_DEV = 128
CAP = 32
EXPERTS = 4
TOKENS = 1024
SLOTS = 256
N_DP = 2


def block_scale(key, dims, cuts, smallest, high):
    def one(position, shards_of):
        draws = jax.random.uniform(jax.random.fold_in(jax.random.fold_in(key, 6), position), (shards_of,), jnp.float32, smallest / len(cuts), high / len(cuts))
        return jnp.repeat(jnp.exp(draws), dims[position] // shards_of).reshape((-1,) + (1,) * (len(dims) - position - 1))

    gain = one(*cuts[0])
    for cut in cuts[1:]:
        gain = gain * one(*cut)
    return gain


def deal_out(own_key, own, number, rows, amount, top, most, lean):
    sequence = jax.random.permutation(own_key, amount)
    heavy_load, common = shares(amount, rows * top, most, lean, True), shares(amount, rows * top, most, lean, False)
    places = jnp.arange(amount)

    def named(sizes, rotation):
        used = int((sizes > 0).sum())
        fixed = max(1, used // 4)
        moved = fixed + (places - fixed + rotation * (used - fixed)) % max(1, amount - fixed)
        return jnp.zeros((amount,), jnp.int32).at[sequence[jnp.where(places < fixed, places, moved)]].set(jnp.asarray(sizes, jnp.int32))

    sizes = jnp.where(number % 4 == 0, named(heavy_load, number // 4), named(common, number - number // 4 - 1))
    mixed = jax.random.permutation(jax.random.fold_in(own, 3), amount)
    donor, taker = mixed[0:amount // 2 * 2:2], mixed[1:amount // 2 * 2:2]
    margin = jnp.minimum(sizes[donor] - 1, most - sizes[taker]) // 2
    margin = jnp.where((donor == sequence[0]) | (taker == sequence[0]) | (sizes[taker] == 0), 0, jnp.maximum(margin, 0))
    moved = jax.random.randint(jax.random.fold_in(own, 4), (amount // 2,), 0, 1 << 20) % (margin + 1)
    sizes = sizes.at[donor].add(-moved).at[taker].add(moved)
    members = jnp.searchsorted(jnp.cumsum(sizes), jnp.arange(rows * top), side="right").astype(jnp.int32)
    listing = members.reshape(top, rows).T
    listing = listing[jax.random.permutation(jax.random.fold_in(own, 1), rows)]
    rotation = jax.random.randint(jax.random.fold_in(own, 2), (rows, 1), 0, top)
    return jnp.take_along_axis(listing, (jnp.arange(top)[None, :] + rotation) % top, axis=1)


def shares(count, total, limit, lean, full):
    loads = [(1 << 20) // math.isqrt(rank ** lean) + 1 for rank in range(1, count + 1)]
    largest = limit if full else min(limit, max(-(-total // count), total * loads[0] // sum(loads)))
    least = 1 if total - largest >= count - 1 else 0
    counts, spare = [largest] + [least] * (count - 1), total - largest - least * (count - 1)
    while spare > 0:
        free = [i for i in range(1, count) if counts[i] < largest] or [i for i in range(1, count) if counts[i] < limit]
        whole, remaining = sum([loads[i] for i in free]), spare
        for i in free:
            more = min(limit - counts[i], max(1, remaining * loads[i] // whole), spare)
            counts[i] = counts[i] + more
            spare = spare - more
    return np.array(counts)


def centred(stream_key, extent, width, bound, cuts=(), kind=jnp.bfloat16):
    factor_of = block_scale(stream_key, extent, cuts, -0.22, 0.18) if cuts else 1.0
    result = jax.random.normal(stream_key, extent, jnp.float32) * width * factor_of
    return jnp.minimum(jnp.maximum(result, -bound), bound).astype(kind)


def setup_inputs(seed: int = 0) -> dict:
    arg_keys = jax.random.split(jax.random.key(seed), 5)
    grad_out = centred(arg_keys[0], (TOKENS, D), 0.03, 0.1875, ((0, 8), (1, 4)))
    expert_ids_keys = jax.random.split(jax.random.fold_in(arg_keys[1], 1), TOKENS // TOK_DEV)
    expert_ids_turns = jax.random.permutation(jax.random.fold_in(arg_keys[1], 3), TOKENS // TOK_DEV)
    expert_ids = jax.vmap(lambda own, number: deal_out(jax.random.fold_in(arg_keys[1], 2), own, number, TOK_DEV, EXPERTS, TOP, TOK_DEV // 2, 2))(expert_ids_keys, expert_ids_turns).reshape((TOKENS, TOP))
    route_gates = jnp.clip(0.1 + 0.9 * jax.random.uniform(arg_keys[2], (TOKENS, TOP), jnp.float32) ** block_scale(arg_keys[2], (TOKENS, TOP), ((0, 8),), -0.2, 0.2), 0.1, 1.0)
    saved_hidden = centred(arg_keys[3], (EXPERTS, SLOTS, FF), 1.0, 6.0, ((0, 4), (1, 2), (2, 4)))
    return dict(grad_out=grad_out, expert_ids=expert_ids, route_gates=route_gates, saved_hidden=saved_hidden)


def slot_table(expert_ids, route_gates, expert_count):
    routes = expert_ids.reshape(-1).astype(jnp.int32)
    weights = route_gates.reshape(-1)
    onehot = (routes[:, None] == jnp.arange(expert_count, dtype=jnp.int32)[None, :]).astype(jnp.int32)
    before = jnp.cumsum(onehot, axis=0) - onehot
    rank = jnp.sum(before * onehot, axis=1)
    target = jnp.where(rank < CAP, routes * CAP + rank, -1)
    match = jnp.arange(expert_count * CAP, dtype=jnp.int32)[:, None] == target[None, :]
    chosen = match.reshape(expert_count * CAP, -1, TOP).any(axis=2)
    slot_gate = jnp.sum(jnp.where(match, weights[None, :], jnp.zeros_like(weights)[None, :]), axis=1)
    return chosen.astype(jnp.bfloat16), slot_gate


def reference(grad_out, expert_ids, route_gates, saved_hidden):
    blocks = N_DP * EXPERTS
    grads = grad_out.reshape(blocks, TOK_DEV, D)
    ids = expert_ids.reshape(blocks, TOK_DEV, TOP)
    gates = route_gates.reshape(blocks, TOK_DEV, TOP)

    def one_block(items):
        grad_block, id_block, gate_block = items
        chosen, slot_gate = slot_table(id_block, gate_block, EXPERTS)
        picked = jnp.dot(chosen, grad_block, preferred_element_type=jnp.float32)
        return (picked * slot_gate[:, None]).astype(jnp.bfloat16).reshape(EXPERTS, CAP, D)

    slots = lax.map(one_block, (grads, ids, gates))
    slots = jnp.transpose(slots, (1, 0, 2, 3)).reshape(EXPERTS, blocks * CAP, D)

    def one_expert(items):
        hidden, expert_grads = items
        summed = lax.dot_general(hidden, expert_grads, (((0,), (0,)), ((), ())), preferred_element_type=jnp.float32)
        return summed.astype(jnp.bfloat16)

    return lax.map(one_expert, (saved_hidden, slots))
```

```python
import functools

import jax
import jax.numpy as jnp
from jax import lax
from jax.experimental import pallas as pl
from jax.experimental.pallas import tpu as pltpu
from jax.sharding import PartitionSpec as P

TOP = 2
CAP = 32
MESH = pl.DeviceIdType.MESH
TN = (((0,), (0,)), ((), ()))


def slot_table(expert_ids, route_gates, expert_count):
    routes = expert_ids.reshape(-1)
    weights = route_gates.reshape(-1)
    onehot = (routes[:, None] == jnp.arange(expert_count, dtype=jnp.int32)[None, :]).astype(
        jnp.int32
    )
    before = jnp.cumsum(onehot, axis=0) - onehot
    rank = jnp.sum(before * onehot, axis=1)
    target = jnp.where(rank < CAP, routes * CAP + rank, -1)
    match = jnp.arange(expert_count * CAP, dtype=jnp.int32)[:, None] == target[None, :]
    chosen = match.reshape(expert_count * CAP, -1, TOP).any(axis=2)
    slot_gate = jnp.sum(
        jnp.where(match, weights[None, :], jnp.zeros_like(weights)[None, :]), axis=1
    )
    return (chosen.astype(jnp.bfloat16), slot_gate)


def plain(grad_out, expert_ids, route_gates, saved_hidden):
    data_count = lax.axis_size("dp")
    expert_count = lax.axis_size("expert")
    chosen, slot_gate = slot_table(expert_ids, route_gates, expert_count)
    width = grad_out.shape[1] * lax.axis_size("tensor")
    block_width = width // data_count
    complete = lax.all_gather(grad_out, "tensor", axis=1, tiled=True)
    parted = complete.reshape(complete.shape[0], data_count, block_width)
    picked = jnp.einsum("st,tdk->dsk", chosen, parted, preferred_element_type=jnp.float32)
    outgoing = (picked * slot_gate[None, :, None]).astype(jnp.bfloat16)
    outgoing = outgoing.reshape(data_count * expert_count, CAP, block_width)
    arrived = lax.all_to_all(outgoing, ("dp", "expert"), split_axis=0, concat_axis=0, tiled=True)
    received = arrived.reshape(-1, block_width)
    summed = lax.dot_general(
        lax.all_gather(saved_hidden[0], "dp", axis=0, tiled=True),
        received,
        TN,
        preferred_element_type=jnp.float32,
    )
    return summed.astype(jnp.bfloat16)[None]


def slot_rows(ids, gates, grad, experts):
    tokens = ids.shape[1]
    named, gate, rank = [], [], []
    for e in range(experts):
        first = (ids[0:1, :] == e).astype(jnp.float32)
        second = (ids[1:2, :] == e).astype(jnp.float32)
        named.append(jnp.broadcast_to(first + second, (CAP, tokens)))
        gate.append(jnp.broadcast_to(first * gates[0:1, :] + second * gates[1:2, :], (CAP, tokens)))
        rank.append(lax.broadcasted_iota(jnp.int32, (CAP, tokens), 0))
    named = jnp.concatenate(named, axis=0)
    gate = jnp.concatenate(gate, axis=0)
    rank = jnp.concatenate(rank, axis=0).astype(jnp.float32)
    row = lax.broadcasted_iota(jnp.int32, (tokens, tokens), 0)
    column = lax.broadcasted_iota(jnp.int32, (tokens, tokens), 1)
    earlier = jnp.where(row < column, 1.0, 0.0).astype(jnp.bfloat16)
    before = jnp.dot(named.astype(jnp.bfloat16), earlier, preferred_element_type=jnp.float32)
    chosen = jnp.where(before == rank, named, 0.0)
    slot_gate = jnp.sum(chosen * gate, axis=1, keepdims=True)
    picked = jnp.dot(chosen.astype(jnp.bfloat16), grad, preferred_element_type=jnp.float32)
    return (picked * slot_gate).astype(jnp.bfloat16)


def exchange(
    D, E, T, cuts, ids_ref, gates_ref, grad_ref, hidden_ref, g_ref, other_ref, slots,
    h_send, h_recv, s1, r1, s2, r2, s3, r3,
):
    d, e, t = lax.axis_index("dp"), lax.axis_index("expert"), lax.axis_index("tensor")
    q = T // D
    x, c = t // q, t % q
    cols = grad_ref.shape[1]
    W = cols // D
    rows = hidden_ref.shape[0]

    def hidden_copy(n, i):
        lo, hi = cuts[i], cuts[i + 1]
        return pltpu.make_async_remote_copy(
            src_ref=hidden_ref.at[pl.ds(lo, hi - lo), :],
            dst_ref=other_ref.at[pl.ds((D - n - 1) * rows + lo, hi - lo), :],
            send_sem=h_send.at[n - 1, i],
            recv_sem=h_recv.at[D - n - 1, i],
            device_id=((d + n) % D, e, t),
            device_id_type=MESH,
        )

    for n in range(1, D):
        hidden_copy(n, 0).start()

    slots[...] = slot_rows(ids_ref[...], gates_ref[...], grad_ref[...], E)

    def place(r, source, x_at, c_at):
        return g_ref.at[
            pl.ds(pl.multiple_of(r * (E * CAP) + source * CAP, CAP), CAP),
            pl.ds(pl.multiple_of(c_at * cols + x_at * W, 128), W),
        ]

    def first(j, m):
        e2, x2 = (e + j) % E, (x + m) % D
        r = (d - x + D) % D
        src = slots.at[
            pl.ds(pl.multiple_of(e2 * CAP, CAP), CAP), pl.ds(pl.multiple_of(x2 * W, 128), W)
        ]
        return src, place(r, e, x2, c), r1.at[r, (E - j) % E], (x, e2, x2 * q + c)

    def first_remote(j, m):
        src, dst, sem, to = first(j, m)
        return pltpu.make_async_remote_copy(
            src_ref=src, dst_ref=dst, send_sem=s1.at[j, m], recv_sem=sem,
            device_id=to, device_id_type=MESH,
        )

    def first_local():
        src = slots.at[
            pl.ds(pl.multiple_of(e * CAP, CAP), CAP), pl.ds(pl.multiple_of(x * W, 128), W)
        ]
        return pltpu.make_async_copy(src, place(0, e, x, c), r1.at[0, 0])

    order = sorted(range(E), key=lambda j: -min(j, E - j))
    for j in order:
        for m in range(D):
            if j == 0 and m == 0:
                pl.when(x == d)(lambda: first_local().start())
                pl.when(x != d)(lambda: first_remote(0, 0).start())
            else:
                first_remote(j, m).start()

    for i in range(1, len(cuts) - 1):
        for n in range(1, D):
            hidden_copy(n, i).start()

    def along(n, r, k):
        here = place(r, (e + k) % E, x, c)
        return pltpu.make_async_remote_copy(
            src_ref=here, dst_ref=here, send_sem=s2.at[n - 1, r, k], recv_sem=r2.at[D - n - 1, r, k],
            device_id=(d, e, ((x + n) % D) * q + c), device_id_type=MESH,
        )

    def along_arrived(n, r, k):
        here = place(r, (e + k) % E, (x + n) % D, c)
        return pltpu.make_async_remote_copy(
            src_ref=here, dst_ref=here, send_sem=s2.at[n - 1, r, k], recv_sem=r2.at[n - 1, r, k],
            device_id=(d, e, ((x + n) % D) * q + c), device_id_type=MESH,
        )

    def across(p, n, r, k):
        here = place(r, (e + k) % E, (x + n) % D, c)
        return pltpu.make_async_remote_copy(
            src_ref=here, dst_ref=here, send_sem=s3.at[p - 1, n, r, k],
            recv_sem=r3.at[q - p - 1, n, r, k],
            device_id=(d, e, x * q + (c + p) % q), device_id_type=MESH,
        )

    def across_arrived(p, n, r, k):
        here = place(r, (e + k) % E, (x + n) % D, (c + p) % q)
        return pltpu.make_async_remote_copy(
            src_ref=here, dst_ref=here, send_sem=s3.at[p - 1, n, r, k],
            recv_sem=r3.at[p - 1, n, r, k],
            device_id=(d, e, x * q + (c + p) % q), device_id_type=MESH,
        )

    def first_arrived(r, k):
        here = place(r, (e + k) % E, x, c)
        return pltpu.make_async_remote_copy(
            src_ref=here, dst_ref=here, send_sem=s1.at[0, 0], recv_sem=r1.at[r, k],
            device_id=((d + r) % D, (e + k) % E, d * q + c), device_id_type=MESH,
        )

    blocks = [(r, k) for k in reversed(order) for r in range(D)]
    for r, k in blocks:
        if r == 0 and k == 0:
            pl.when(x == d)(lambda: first_local().wait())
            pl.when(x != d)(lambda: first_arrived(0, 0).wait_recv())
        else:
            first_arrived(r, k).wait_recv()
        for n in range(1, D):
            along(n, r, k).start()
        for p in range(1, q):
            across(p, 0, r, k).start()
    for r, k in blocks:
        for n in range(1, D):
            along_arrived(n, r, k).wait_recv()
            for p in range(1, q):
                across(p, n, r, k).start()
    for r, k in blocks:
        for p in range(1, q):
            for n in range(D):
                across_arrived(p, n, r, k).wait_recv()
    for j in order:
        for m in range(D):
            if j == 0 and m == 0:
                pl.when(x != d)(lambda: first_remote(0, 0).wait_send())
            else:
                first_remote(j, m).wait_send()
    for r, k in blocks:
        for n in range(1, D):
            along(n, r, k).wait_send()
        for p in range(1, q):
            for n in range(D):
                across(p, n, r, k).wait_send()
    for i in range(len(cuts) - 1):
        for n in range(1, D):
            hidden_copy(n, i).wait_send()
            pltpu.make_async_remote_copy(
                src_ref=hidden_ref.at[pl.ds(cuts[i], cuts[i + 1] - cuts[i]), :],
                dst_ref=other_ref.at[pl.ds((n - 1) * rows + cuts[i], cuts[i + 1] - cuts[i]), :],
                send_sem=h_send.at[n - 1, i],
                recv_sem=h_recv.at[n - 1, i],
                device_id=((d + n) % D, e, t),
                device_id_type=MESH,
            ).wait_recv()


def product(strip, own_ref, other_ref, g_ref, o_ref):
    hidden = jnp.concatenate([own_ref[...], other_ref[...]], axis=0)
    for lo in range(0, g_ref.shape[1], strip):
        o_ref[:, lo:lo + strip] = lax.dot_general(
            hidden, g_ref[:, lo:lo + strip], TN, preferred_element_type=jnp.float32
        ).astype(o_ref.dtype)


def local(grad_out, expert_ids, route_gates, saved_hidden):
    D, E, T = lax.axis_size("dp"), lax.axis_size("expert"), lax.axis_size("tensor")
    tokens, cols = grad_out.shape
    rows, units = saved_hidden.shape[1:]
    depth = D * E * CAP
    width = cols * T // D
    tile, strip = 512, 1024
    if T % D or cols % (128 * D) or units % tile or width % strip or rows != E * CAP or tokens % 128:
        return plain(grad_out, expert_ids, route_gates, saved_hidden)
    q = T // D
    hidden = saved_hidden[0]
    cuts = (0, rows // 4, rows)
    pieces = len(cuts) - 1
    vmem = pl.BlockSpec(memory_space=pltpu.VMEM)
    hbm = pl.BlockSpec(memory_space=pl.ANY)
    dma = pltpu.SemaphoreType.DMA
    g, other = pl.pallas_call(
        functools.partial(exchange, D, E, T, cuts),
        out_shape=(
            jax.ShapeDtypeStruct((depth, width), jnp.bfloat16),
            jax.ShapeDtypeStruct(((D - 1) * rows, units), jnp.bfloat16),
        ),
        in_specs=[vmem, vmem, vmem, hbm],
        out_specs=(vmem, hbm),
        scratch_shapes=[
            pltpu.VMEM((E * CAP, cols), jnp.bfloat16),
            dma((D - 1, pieces)), dma((D - 1, pieces)),
            dma((E, D)), dma((D, E)),
            dma((D - 1, D, E)), dma((D - 1, D, E)),
            dma((q - 1, D, D, E)), dma((q - 1, D, D, E)),
        ],
        compiler_params=pltpu.CompilerParams(has_side_effects=True),
    )(expert_ids.T, route_gates.T, grad_out, hidden)
    summed = pl.pallas_call(
        functools.partial(product, strip),
        grid=(units // tile,),
        out_shape=jax.ShapeDtypeStruct((units, width), jnp.bfloat16),
        in_specs=[
            pl.BlockSpec((rows, tile), lambda i: (0, i)),
            pl.BlockSpec(((D - 1) * rows, tile), lambda i: (0, i)),
            pl.BlockSpec((depth, width), lambda i: (0, 0)),
        ],
        out_specs=pl.BlockSpec((tile, width), lambda i: (i, 0)),
        compiler_params=pltpu.CompilerParams(dimension_semantics=("arbitrary",)),
    )(hidden, other, g)
    return summed[None]


def solution(mesh):
    in_specs = (
        P(("dp", "expert"), "tensor"),
        P(("dp", "expert"), None),
        P(("dp", "expert"), None),
        P("expert", "dp", "tensor"),
    )
    out_specs = P("expert", "tensor", "dp")
    return jax.shard_map(local, mesh=mesh, in_specs=in_specs, out_specs=out_specs, check_vma=False)
```

```python
import functools

import jax
import jax.numpy as jnp
from jax import lax
from jax.experimental import pallas as pl
from jax.experimental.pallas import tpu as pltpu
from jax.sharding import PartitionSpec as P

TOP = 2
CAP = 32
MESH = pl.DeviceIdType.MESH
TN = (((0,), (0,)), ((), ()))


def slot_table(expert_ids, route_gates, expert_count):
    routes = expert_ids.reshape(-1)
    weights = route_gates.reshape(-1)
    onehot = (routes[:, None] == jnp.arange(expert_count, dtype=jnp.int32)[None, :]).astype(
        jnp.int32
    )
    before = jnp.cumsum(onehot, axis=0) - onehot
    rank = jnp.sum(before * onehot, axis=1)
    target = jnp.where(rank < CAP, routes * CAP + rank, -1)
    match = jnp.arange(expert_count * CAP, dtype=jnp.int32)[:, None] == target[None, :]
    chosen = match.reshape(expert_count * CAP, -1, TOP).any(axis=2)
    slot_gate = jnp.sum(
        jnp.where(match, weights[None, :], jnp.zeros_like(weights)[None, :]), axis=1
    )
    return (chosen.astype(jnp.bfloat16), slot_gate)


def plain(grad_out, expert_ids, route_gates, saved_hidden):
    data_count = lax.axis_size("dp")
    expert_count = lax.axis_size("expert")
    chosen, slot_gate = slot_table(expert_ids, route_gates, expert_count)
    width = grad_out.shape[1] * lax.axis_size("tensor")
    block_width = width // data_count
    complete = lax.all_gather(grad_out, "tensor", axis=1, tiled=True)
    parted = complete.reshape(complete.shape[0], data_count, block_width)
    picked = jnp.einsum("st,tdk->dsk", chosen, parted, preferred_element_type=jnp.float32)
    outgoing = (picked * slot_gate[None, :, None]).astype(jnp.bfloat16)
    outgoing = outgoing.reshape(data_count * expert_count, CAP, block_width)
    arrived = lax.all_to_all(outgoing, ("dp", "expert"), split_axis=0, concat_axis=0, tiled=True)
    received = arrived.reshape(-1, block_width)
    summed = lax.dot_general(
        lax.all_gather(saved_hidden[0], "dp", axis=0, tiled=True),
        received,
        TN,
        preferred_element_type=jnp.float32,
    )
    return summed.astype(jnp.bfloat16)[None]


def slot_rows(ids, gates, grad, experts):
    tokens = ids.shape[1]
    named, gate, rank = [], [], []
    for e in range(experts):
        first = (ids[0:1, :] == e).astype(jnp.float32)
        second = (ids[1:2, :] == e).astype(jnp.float32)
        named.append(jnp.broadcast_to(first + second, (CAP, tokens)))
        gate.append(jnp.broadcast_to(first * gates[0:1, :] + second * gates[1:2, :], (CAP, tokens)))
        rank.append(lax.broadcasted_iota(jnp.int32, (CAP, tokens), 0))
    named = jnp.concatenate(named, axis=0)
    gate = jnp.concatenate(gate, axis=0)
    rank = jnp.concatenate(rank, axis=0).astype(jnp.float32)
    row = lax.broadcasted_iota(jnp.int32, (tokens, tokens), 0)
    column = lax.broadcasted_iota(jnp.int32, (tokens, tokens), 1)
    earlier = jnp.where(row < column, 1.0, 0.0).astype(jnp.bfloat16)
    before = jnp.dot(named.astype(jnp.bfloat16), earlier, preferred_element_type=jnp.float32)
    chosen = jnp.where(before == rank, named, 0.0)
    slot_gate = jnp.sum(chosen * gate, axis=1, keepdims=True)
    picked = jnp.dot(chosen.astype(jnp.bfloat16), grad, preferred_element_type=jnp.float32)
    return (picked * slot_gate).astype(jnp.bfloat16)


def exchange(
    D, E, T, cuts, ids_ref, gates_ref, grad_ref, hidden_ref, g_ref, other_ref, slots,
    h_send, h_recv, s1, r1, s2, r2, s3, r3,
):
    d, e, t = lax.axis_index("dp"), lax.axis_index("expert"), lax.axis_index("tensor")
    q = T // D
    x, c = t // q, t % q
    cols = grad_ref.shape[1]
    W = cols // D
    rows = hidden_ref.shape[0]

    def hidden_copy(n, i):
        lo, hi = cuts[i], cuts[i + 1]
        return pltpu.make_async_remote_copy(
            src_ref=hidden_ref.at[pl.ds(lo, hi - lo), :],
            dst_ref=other_ref.at[pl.ds((D - n - 1) * rows + lo, hi - lo), :],
            send_sem=h_send.at[n - 1, i],
            recv_sem=h_recv.at[D - n - 1, i],
            device_id=((d + n) % D, e, t),
            device_id_type=MESH,
        )

    for n in range(1, D):
        hidden_copy(n, 0).start()

    slots[...] = slot_rows(ids_ref[...], gates_ref[...], grad_ref[...], E)

    def place(r, source, x_at, c_at):
        return g_ref.at[
            pl.ds(pl.multiple_of(r * (E * CAP) + source * CAP, CAP), CAP),
            pl.ds(pl.multiple_of(c_at * cols + x_at * W, 128), W),
        ]

    def first(j, m):
        e2, x2 = (e + j) % E, (x + m) % D
        r = (d - x + D) % D
        src = slots.at[
            pl.ds(pl.multiple_of(e2 * CAP, CAP), CAP), pl.ds(pl.multiple_of(x2 * W, 128), W)
        ]
        return src, place(r, e, x2, c), r1.at[r, (E - j) % E], (x, e2, x2 * q + c)

    def first_remote(j, m):
        src, dst, sem, to = first(j, m)
        return pltpu.make_async_remote_copy(
            src_ref=src, dst_ref=dst, send_sem=s1.at[j, m], recv_sem=sem,
            device_id=to, device_id_type=MESH,
        )

    def first_local():
        src = slots.at[
            pl.ds(pl.multiple_of(e * CAP, CAP), CAP), pl.ds(pl.multiple_of(x * W, 128), W)
        ]
        return pltpu.make_async_copy(src, place(0, e, x, c), r1.at[0, 0])

    order = sorted(range(E), key=lambda j: -min(j, E - j))
    for j in order:
        for m in range(D):
            if j == 0 and m == 0:
                pl.when(x == d)(lambda: first_local().start())
                pl.when(x != d)(lambda: first_remote(0, 0).start())
            else:
                first_remote(j, m).start()

    for i in range(1, len(cuts) - 1):
        for n in range(1, D):
            hidden_copy(n, i).start()

    def along(n, r, k):
        here = place(r, (e + k) % E, x, c)
        return pltpu.make_async_remote_copy(
            src_ref=here, dst_ref=here, send_sem=s2.at[n - 1, r, k], recv_sem=r2.at[D - n - 1, r, k],
            device_id=(d, e, ((x + n) % D) * q + c), device_id_type=MESH,
        )

    def along_arrived(n, r, k):
        here = place(r, (e + k) % E, (x + n) % D, c)
        return pltpu.make_async_remote_copy(
            src_ref=here, dst_ref=here, send_sem=s2.at[n - 1, r, k], recv_sem=r2.at[n - 1, r, k],
            device_id=(d, e, ((x + n) % D) * q + c), device_id_type=MESH,
        )

    def across(p, n, r, k):
        here = place(r, (e + k) % E, (x + n) % D, c)
        return pltpu.make_async_remote_copy(
            src_ref=here, dst_ref=here, send_sem=s3.at[p - 1, n, r, k],
            recv_sem=r3.at[q - p - 1, n, r, k],
            device_id=(d, e, x * q + (c + p) % q), device_id_type=MESH,
        )

    def across_arrived(p, n, r, k):
        here = place(r, (e + k) % E, (x + n) % D, (c + p) % q)
        return pltpu.make_async_remote_copy(
            src_ref=here, dst_ref=here, send_sem=s3.at[p - 1, n, r, k],
            recv_sem=r3.at[p - 1, n, r, k],
            device_id=(d, e, x * q + (c + p) % q), device_id_type=MESH,
        )

    def first_arrived(r, k):
        here = place(r, (e + k) % E, x, c)
        return pltpu.make_async_remote_copy(
            src_ref=here, dst_ref=here, send_sem=s1.at[0, 0], recv_sem=r1.at[r, k],
            device_id=((d + r) % D, (e + k) % E, d * q + c), device_id_type=MESH,
        )

    blocks = [(r, k) for k in reversed(order) for r in range(D)]
    for r, k in blocks:
        if r == 0 and k == 0:
            pl.when(x == d)(lambda: first_local().wait())
            pl.when(x != d)(lambda: first_arrived(0, 0).wait_recv())
        else:
            first_arrived(r, k).wait_recv()
        for n in range(1, D):
            along(n, r, k).start()
        for p in range(1, q):
            across(p, 0, r, k).start()
    for r, k in blocks:
        for n in range(1, D):
            along_arrived(n, r, k).wait_recv()
            for p in range(1, q):
                across(p, n, r, k).start()
    for r, k in blocks:
        for p in range(1, q):
            for n in range(D):
                across_arrived(p, n, r, k).wait_recv()
    for j in order:
        for m in range(D):
            if j == 0 and m == 0:
                pl.when(x != d)(lambda: first_remote(0, 0).wait_send())
            else:
                first_remote(j, m).wait_send()
    for r, k in blocks:
        for n in range(1, D):
            along(n, r, k).wait_send()
        for p in range(1, q):
            for n in range(D):
                across(p, n, r, k).wait_send()
    for i in range(len(cuts) - 1):
        for n in range(1, D):
            hidden_copy(n, i).wait_send()
            pltpu.make_async_remote_copy(
                src_ref=hidden_ref.at[pl.ds(cuts[i], cuts[i + 1] - cuts[i]), :],
                dst_ref=other_ref.at[pl.ds((n - 1) * rows + cuts[i], cuts[i + 1] - cuts[i]), :],
                send_sem=h_send.at[n - 1, i],
                recv_sem=h_recv.at[n - 1, i],
                device_id=((d + n) % D, e, t),
                device_id_type=MESH,
            ).wait_recv()


def product(strip, own_ref, other_ref, g_ref, o_ref):
    hidden = jnp.concatenate([own_ref[...], other_ref[...]], axis=0)
    for lo in range(0, g_ref.shape[1], strip):
        o_ref[:, lo:lo + strip] = lax.dot_general(
            hidden, g_ref[:, lo:lo + strip], TN, preferred_element_type=jnp.float32
        ).astype(o_ref.dtype)


def local(grad_out, expert_ids, route_gates, saved_hidden):
    D, E, T = lax.axis_size("dp"), lax.axis_size("expert"), lax.axis_size("tensor")
    tokens, cols = grad_out.shape
    rows, units = saved_hidden.shape[1:]
    depth = D * E * CAP
    width = cols * T // D
    tile, strip = 1024, 1024
    if T % D or cols % (128 * D) or units % tile or width % strip or rows != E * CAP or tokens % 128:
        return plain(grad_out, expert_ids, route_gates, saved_hidden)
    q = T // D
    hidden = saved_hidden[0]
    cuts = (0, rows // 4, rows)
    pieces = len(cuts) - 1
    vmem = pl.BlockSpec(memory_space=pltpu.VMEM)
    hbm = pl.BlockSpec(memory_space=pl.ANY)
    dma = pltpu.SemaphoreType.DMA
    g, other = pl.pallas_call(
        functools.partial(exchange, D, E, T, cuts),
        out_shape=(
            jax.ShapeDtypeStruct((depth, width), jnp.bfloat16),
            jax.ShapeDtypeStruct(((D - 1) * rows, units), jnp.bfloat16),
        ),
        in_specs=[vmem, vmem, vmem, hbm],
        out_specs=(vmem, hbm),
        scratch_shapes=[
            pltpu.VMEM((E * CAP, cols), jnp.bfloat16),
            dma((D - 1, pieces)), dma((D - 1, pieces)),
            dma((E, D)), dma((D, E)),
            dma((D - 1, D, E)), dma((D - 1, D, E)),
            dma((q - 1, D, D, E)), dma((q - 1, D, D, E)),
        ],
        compiler_params=pltpu.CompilerParams(has_side_effects=True),
    )(expert_ids.T, route_gates.T, grad_out, hidden)
    summed = pl.pallas_call(
        functools.partial(product, strip),
        grid=(units // tile,),
        out_shape=jax.ShapeDtypeStruct((units, width), jnp.bfloat16),
        in_specs=[
            pl.BlockSpec((rows, tile), lambda i: (0, i)),
            pl.BlockSpec(((D - 1) * rows, tile), lambda i: (0, i)),
            pl.BlockSpec((depth, width), lambda i: (0, 0)),
        ],
        out_specs=pl.BlockSpec((tile, width), lambda i: (i, 0)),
        compiler_params=pltpu.CompilerParams(dimension_semantics=("arbitrary",)),
    )(hidden, other, g)
    return summed[None]


def solution(mesh):
    in_specs = (
        P(("dp", "expert"), "tensor"),
        P(("dp", "expert"), None),
        P(("dp", "expert"), None),
        P("expert", "dp", "tensor"),
    )
    out_specs = P("expert", "tensor", "dp")
    return jax.shard_map(local, mesh=mesh, in_specs=in_specs, out_specs=out_specs, check_vma=False)
```

```python
import functools

import jax
import jax.numpy as jnp
from jax import lax
from jax.experimental import pallas as pl
from jax.experimental.pallas import tpu as pltpu
from jax.sharding import PartitionSpec as P

TOP = 2
CAP = 32
MESH = pl.DeviceIdType.MESH
TN = (((0,), (0,)), ((), ()))


def slot_table(expert_ids, route_gates, expert_count):
    routes = expert_ids.reshape(-1)
    weights = route_gates.reshape(-1)
    onehot = (routes[:, None] == jnp.arange(expert_count, dtype=jnp.int32)[None, :]).astype(
        jnp.int32
    )
    before = jnp.cumsum(onehot, axis=0) - onehot
    rank = jnp.sum(before * onehot, axis=1)
    target = jnp.where(rank < CAP, routes * CAP + rank, -1)
    match = jnp.arange(expert_count * CAP, dtype=jnp.int32)[:, None] == target[None, :]
    chosen = match.reshape(expert_count * CAP, -1, TOP).any(axis=2)
    slot_gate = jnp.sum(
        jnp.where(match, weights[None, :], jnp.zeros_like(weights)[None, :]), axis=1
    )
    return (chosen.astype(jnp.bfloat16), slot_gate)


def plain(grad_out, expert_ids, route_gates, saved_hidden):
    data_count = lax.axis_size("dp")
    expert_count = lax.axis_size("expert")
    chosen, slot_gate = slot_table(expert_ids, route_gates, expert_count)
    width = grad_out.shape[1] * lax.axis_size("tensor")
    block_width = width // data_count
    complete = lax.all_gather(grad_out, "tensor", axis=1, tiled=True)
    parted = complete.reshape(complete.shape[0], data_count, block_width)
    picked = jnp.einsum("st,tdk->dsk", chosen, parted, preferred_element_type=jnp.float32)
    outgoing = (picked * slot_gate[None, :, None]).astype(jnp.bfloat16)
    outgoing = outgoing.reshape(data_count * expert_count, CAP, block_width)
    arrived = lax.all_to_all(outgoing, ("dp", "expert"), split_axis=0, concat_axis=0, tiled=True)
    received = arrived.reshape(-1, block_width)
    summed = lax.dot_general(
        lax.all_gather(saved_hidden[0], "dp", axis=0, tiled=True),
        received,
        TN,
        preferred_element_type=jnp.float32,
    )
    return summed.astype(jnp.bfloat16)[None]


def slot_rows(ids, gates, grad, experts):
    tokens = ids.shape[1]
    named, gate, rank = [], [], []
    for e in range(experts):
        first = (ids[0:1, :] == e).astype(jnp.float32)
        second = (ids[1:2, :] == e).astype(jnp.float32)
        named.append(jnp.broadcast_to(first + second, (CAP, tokens)))
        gate.append(jnp.broadcast_to(first * gates[0:1, :] + second * gates[1:2, :], (CAP, tokens)))
        rank.append(lax.broadcasted_iota(jnp.int32, (CAP, tokens), 0))
    named = jnp.concatenate(named, axis=0)
    gate = jnp.concatenate(gate, axis=0)
    rank = jnp.concatenate(rank, axis=0).astype(jnp.float32)
    row = lax.broadcasted_iota(jnp.int32, (tokens, tokens), 0)
    column = lax.broadcasted_iota(jnp.int32, (tokens, tokens), 1)
    earlier = jnp.where(row < column, 1.0, 0.0).astype(jnp.bfloat16)
    before = jnp.dot(named.astype(jnp.bfloat16), earlier, preferred_element_type=jnp.float32)
    chosen = jnp.where(before == rank, named, 0.0)
    slot_gate = jnp.sum(chosen * gate, axis=1, keepdims=True)
    picked = jnp.dot(chosen.astype(jnp.bfloat16), grad, preferred_element_type=jnp.float32)
    return (picked * slot_gate).astype(jnp.bfloat16)


def exchange(
    D, E, T, cuts, ids_ref, gates_ref, grad_ref, hidden_ref, g_ref, other_ref, slots,
    h_send, h_recv, s1, r1, s2, r2, s3, r3,
):
    d, e, t = lax.axis_index("dp"), lax.axis_index("expert"), lax.axis_index("tensor")
    q = T // D
    x, c = t // q, t % q
    cols = grad_ref.shape[1]
    W = cols // D
    rows, kept = hidden_ref.shape[0], other_ref.shape[1]

    def hidden_copy(n, i):
        lo, hi = cuts[i], cuts[i + 1]
        return pltpu.make_async_remote_copy(
            src_ref=hidden_ref.at[pl.ds(lo, hi - lo), pl.ds(0, kept)],
            dst_ref=other_ref.at[pl.ds((D - n - 1) * rows + lo, hi - lo), :],
            send_sem=h_send.at[n - 1, i],
            recv_sem=h_recv.at[D - n - 1, i],
            device_id=((d + n) % D, e, t),
            device_id_type=MESH,
        )

    for n in range(1, D):
        hidden_copy(n, 0).start()

    slots[...] = slot_rows(ids_ref[...], gates_ref[...], grad_ref[...], E)

    def place(r, source, x_at, c_at):
        return g_ref.at[
            pl.ds(pl.multiple_of(r * (E * CAP) + source * CAP, CAP), CAP),
            pl.ds(pl.multiple_of(c_at * cols + x_at * W, 128), W),
        ]

    def first(j, m):
        e2, x2 = (e + j) % E, (x + m) % D
        r = (d - x + D) % D
        src = slots.at[
            pl.ds(pl.multiple_of(e2 * CAP, CAP), CAP), pl.ds(pl.multiple_of(x2 * W, 128), W)
        ]
        return src, place(r, e, x2, c), r1.at[r, (E - j) % E], (x, e2, x2 * q + c)

    def first_remote(j, m):
        src, dst, sem, to = first(j, m)
        return pltpu.make_async_remote_copy(
            src_ref=src, dst_ref=dst, send_sem=s1.at[j, m], recv_sem=sem,
            device_id=to, device_id_type=MESH,
        )

    def first_local():
        src = slots.at[
            pl.ds(pl.multiple_of(e * CAP, CAP), CAP), pl.ds(pl.multiple_of(x * W, 128), W)
        ]
        return pltpu.make_async_copy(src, place(0, e, x, c), r1.at[0, 0])

    order = sorted(range(E), key=lambda j: -min(j, E - j))
    for j in order:
        for m in range(D):
            if j == 0 and m == 0:
                pl.when(x == d)(lambda: first_local().start())
                pl.when(x != d)(lambda: first_remote(0, 0).start())
            else:
                first_remote(j, m).start()

    for i in range(1, len(cuts) - 1):
        for n in range(1, D):
            hidden_copy(n, i).start()

    def along(n, r, k):
        here = place(r, (e + k) % E, x, c)
        return pltpu.make_async_remote_copy(
            src_ref=here, dst_ref=here, send_sem=s2.at[n - 1, r, k], recv_sem=r2.at[D - n - 1, r, k],
            device_id=(d, e, ((x + n) % D) * q + c), device_id_type=MESH,
        )

    def along_arrived(n, r, k):
        here = place(r, (e + k) % E, (x + n) % D, c)
        return pltpu.make_async_remote_copy(
            src_ref=here, dst_ref=here, send_sem=s2.at[n - 1, r, k], recv_sem=r2.at[n - 1, r, k],
            device_id=(d, e, ((x + n) % D) * q + c), device_id_type=MESH,
        )

    def across(p, n, r, k):
        here = place(r, (e + k) % E, (x + n) % D, c)
        return pltpu.make_async_remote_copy(
            src_ref=here, dst_ref=here, send_sem=s3.at[p - 1, n, r, k],
            recv_sem=r3.at[q - p - 1, n, r, k],
            device_id=(d, e, x * q + (c + p) % q), device_id_type=MESH,
        )

    def across_arrived(p, n, r, k):
        here = place(r, (e + k) % E, (x + n) % D, (c + p) % q)
        return pltpu.make_async_remote_copy(
            src_ref=here, dst_ref=here, send_sem=s3.at[p - 1, n, r, k],
            recv_sem=r3.at[p - 1, n, r, k],
            device_id=(d, e, x * q + (c + p) % q), device_id_type=MESH,
        )

    def first_arrived(r, k):
        here = place(r, (e + k) % E, x, c)
        return pltpu.make_async_remote_copy(
            src_ref=here, dst_ref=here, send_sem=s1.at[0, 0], recv_sem=r1.at[r, k],
            device_id=((d + r) % D, (e + k) % E, d * q + c), device_id_type=MESH,
        )

    blocks = [(r, k) for k in reversed(order) for r in range(D)]
    for r, k in blocks:
        if r == 0 and k == 0:
            pl.when(x == d)(lambda: first_local().wait())
            pl.when(x != d)(lambda: first_arrived(0, 0).wait_recv())
        else:
            first_arrived(r, k).wait_recv()
        for n in range(1, D):
            along(n, r, k).start()
        for p in range(1, q):
            across(p, 0, r, k).start()
    for r, k in blocks:
        for n in range(1, D):
            along_arrived(n, r, k).wait_recv()
            for p in range(1, q):
                across(p, n, r, k).start()
    for r, k in blocks:
        for p in range(1, q):
            for n in range(D):
                across_arrived(p, n, r, k).wait_recv()
    for j in order:
        for m in range(D):
            if j == 0 and m == 0:
                pl.when(x != d)(lambda: first_remote(0, 0).wait_send())
            else:
                first_remote(j, m).wait_send()
    for r, k in blocks:
        for n in range(1, D):
            along(n, r, k).wait_send()
        for p in range(1, q):
            for n in range(D):
                across(p, n, r, k).wait_send()
    for i in range(len(cuts) - 1):
        for n in range(1, D):
            hidden_copy(n, i).wait_send()
            pltpu.make_async_remote_copy(
                src_ref=hidden_ref.at[pl.ds(cuts[i], cuts[i + 1] - cuts[i]), pl.ds(0, kept)],
                dst_ref=other_ref.at[pl.ds((n - 1) * rows + cuts[i], cuts[i + 1] - cuts[i]), :],
                send_sem=h_send.at[n - 1, i],
                recv_sem=h_recv.at[n - 1, i],
                device_id=((d + n) % D, e, t),
                device_id_type=MESH,
            ).wait_recv()


def product(strip, own_ref, other_ref, g_ref, o_ref):
    hidden = jnp.concatenate([own_ref[...], other_ref[...]], axis=0)
    for lo in range(0, g_ref.shape[1], strip):
        o_ref[:, lo:lo + strip] = lax.dot_general(
            hidden, g_ref[:, lo:lo + strip], TN, preferred_element_type=jnp.float32
        ).astype(o_ref.dtype)


def local(grad_out, expert_ids, route_gates, saved_hidden):
    D, E, T = lax.axis_size("dp"), lax.axis_size("expert"), lax.axis_size("tensor")
    tokens, cols = grad_out.shape
    rows, units = saved_hidden.shape[1:]
    depth = D * E * CAP
    width = cols * T // D
    tile, strip = 1024, 1024
    if T % D or cols % (128 * D) or units % tile or units == tile or width % strip or rows != E * CAP or tokens % 128:
        return plain(grad_out, expert_ids, route_gates, saved_hidden)
    q = T // D
    hidden = saved_hidden[0]
    cuts = (0, rows // 4, rows)
    pieces = len(cuts) - 1
    vmem = pl.BlockSpec(memory_space=pltpu.VMEM)
    hbm = pl.BlockSpec(memory_space=pl.ANY)
    dma = pltpu.SemaphoreType.DMA
    g, other = pl.pallas_call(
        functools.partial(exchange, D, E, T, cuts),
        out_shape=(
            jax.ShapeDtypeStruct((depth, width), jnp.bfloat16),
            jax.ShapeDtypeStruct(((D - 1) * rows, units - tile), jnp.bfloat16),
        ),
        in_specs=[vmem, vmem, vmem, hbm],
        out_specs=(vmem, hbm),
        scratch_shapes=[
            pltpu.VMEM((E * CAP, cols), jnp.bfloat16),
            dma((D - 1, pieces)), dma((D - 1, pieces)),
            dma((E, D)), dma((D, E)),
            dma((D - 1, D, E)), dma((D - 1, D, E)),
            dma((q - 1, D, D, E)), dma((q - 1, D, D, E)),
        ],
        compiler_params=pltpu.CompilerParams(has_side_effects=True),
    )(expert_ids.T, route_gates.T, grad_out, hidden)
    tail, g, other = lax.optimization_barrier((hidden[:, units - tile:], g, other))
    moved = jnp.concatenate(
        [lax.ppermute(tail, "dp", [(s, (s - n) % D) for s in range(D)]) for n in range(1, D)]
    )

    def multiply(first, count, other_part, *into):
        return pl.pallas_call(
            lambda own_ref, other_ref, g_ref, *rest: product(
                strip, own_ref, other_ref, g_ref, rest[-1]
            ),
            grid=(count,),
            out_shape=jax.ShapeDtypeStruct((units, width), jnp.bfloat16),
            in_specs=[
                pl.BlockSpec((rows, tile), lambda i: (0, first + i)),
                pl.BlockSpec(((D - 1) * rows, tile), lambda i: (0, i)),
                pl.BlockSpec((depth, width), lambda i: (0, 0)),
            ] + [hbm] * len(into),
            out_specs=pl.BlockSpec((tile, width), lambda i: (first + i, 0)),
            input_output_aliases={3: 0} if into else {},
            compiler_params=pltpu.CompilerParams(dimension_semantics=("arbitrary",)),
            cost_estimate=pl.CostEstimate(
                flops=2 * count * tile * width * depth,
                bytes_accessed=2 * count * tile * width,
                transcendentals=0,
            ),
        )(hidden, other_part, g, *into)

    begun = multiply(0, units // tile - 1, other)
    summed = multiply(units // tile - 1, 1, moved, begun)
    return summed[None]


def solution(mesh):
    in_specs = (
        P(("dp", "expert"), "tensor"),
        P(("dp", "expert"), None),
        P(("dp", "expert"), None),
        P("expert", "dp", "tensor"),
    )
    out_specs = P("expert", "tensor", "dp")
    return jax.shard_map(local, mesh=mesh, in_specs=in_specs, out_specs=out_specs, check_vma=False)
```
